128 devices in a mesh: dp: 8 (over x, core), mp: 16 (over y, z).
Axes of the slice: x: 4, y: 4, z: 4, core: 2. Of those that a mesh axis runs over, the one named last changes fastest.
Arguments:
- tokens: bfloat16 [256, 8192], P('dp', 'mp'), may hold values from -6 to 6
- gate_up_weight: bfloat16 [2, 8192, 15360], P(None, 'mp', 'dp'), may hold values from -0.0625 to 0.0625
- down_weight: bfloat16 [15360, 8192], P('dp', 'mp'), may hold values from -0.046875 to 0.046875
- gate_up_input_factor: bfloat16 [2, 8192, 64], P(None, 'mp'), may hold values from -0.0625 to 0.0625
- gate_up_output_factor: bfloat16 [2, 64, 15360], P(None, None, 'dp'), may hold values from -0.046875 to 0.046875
- down_input_factor: bfloat16 [15360, 64], P('dp'), may hold values from -0.046875 to 0.046875
- down_output_factor: bfloat16 [64, 8192], P(None, 'mp'), may hold values from -0.0625 to 0.0625
- cotangent: bfloat16 [256, 8192], P('dp', 'mp'), may hold values from -6 to 6
Outputs:
- output: bfloat16 [256, 8192], P('dp', 'mp')
- input_grad: bfloat16 [256, 8192], P('dp', 'mp')
- grad_gate_up_lower: float32 [2, 8192, 64], P(None, 'mp')
- gate_up_output_factor_gradient: float32 [2, 64, 15360], P(None, None, 'dp')
- down_input_factor_gradient: float32 [15360, 64], P('dp')
- down_output_factor_gradient: float32 [64, 8192], P(None, 'mp')
The draws below stay inside these ranges and needn't reach their ends.
All inputs are finite; a program needn't handle non-finite values.
Results may differ from the reference program's by a relative error of at most 0.0065.
Values may be sent and summed in bfloat16 or wider, within the bound.
No kernel may reach another device: no remote copies, remote signals or barrier semaphores. Data moves between devices by JAX's collectives and lax.ppermute only.
A program may use at most 64 MiB of HBM per device.

```python
import jax
import jax.numpy as jnp
from jax import lax

D = 8192
FF = 15360
R = 64
TOKENS = 256


def steps_of(key, dims, cuts, low, high):
    loudness = 1.0
    for dim, parts in cuts:
        draws = jax.random.uniform(jax.random.fold_in(jax.random.fold_in(key, 6), dim), (parts,), jnp.float32, low / len(cuts), high / len(cuts))
        loudness = loudness * jnp.repeat(jnp.exp(draws), dims[dim] // parts).reshape((-1,) + (1,) * (len(dims) - 1 - dim))
    return loudness


def normal_values(stream_key, shape, width, bound, split=(), dtype=jnp.bfloat16):
    gain = steps_of(stream_key, shape, split, -0.22, 0.18) if split else 1.0
    values = jax.random.normal(stream_key, shape, jnp.float32) * width * gain
    return jnp.minimum(jnp.maximum(values, -bound), bound).astype(dtype)


def setup_inputs(seed: int = 0) -> dict:
    key_of = jax.random.split(jax.random.key(seed), 9)
    tokens = normal_values(key_of[0], (TOKENS, D), 1.0, 6.0, ((0, 8), (1, 16)))
    gate_up_weight = normal_values(key_of[1], (2, D, FF), D ** -0.5, 0.0625, ((1, 16), (2, 8)))
    down_weight = normal_values(key_of[2], (FF, D), FF ** -0.5, 0.046875, ((0, 8), (1, 16)))
    gate_up_input_factor = normal_values(key_of[3], (2, D, R), D ** -0.5, 0.0625, ((1, 16),))
    gate_up_output_factor = normal_values(key_of[4], (2, R, FF), FF ** -0.5, 0.046875, ((2, 8),))
    down_input_factor = normal_values(key_of[5], (FF, R), FF ** -0.5, 0.046875, ((0, 8),))
    down_output_factor = normal_values(key_of[6], (R, D), D ** -0.5, 0.0625, ((1, 16),))
    cotangent = normal_values(key_of[7], (TOKENS, D), 1.0, 6.0, ((0, 8), (1, 16)))
    return {"tokens": tokens, "gate_up_weight": gate_up_weight, "down_weight": down_weight, "gate_up_input_factor": gate_up_input_factor, "gate_up_output_factor": gate_up_output_factor, "down_input_factor": down_input_factor, "down_output_factor": down_output_factor, "cotangent": cotangent}


adapter_scale = 2.0


def reference(tokens, gate_up_weight, down_weight, gate_up_input_factor, gate_up_output_factor, down_input_factor, down_output_factor, cotangent):
    single_float = jnp.float32
    upper_projection = lax.Precision.HIGHEST
    scale_factor = TOKENS ** -0.5
    lower_results = []
    pres = []
    for rank_dimension in range(2):
        lower_projection = jnp.dot(tokens, gate_up_input_factor[rank_dimension], preferred_element_type=single_float)
        lower_results.append(lower_projection)
        preactivation = jnp.dot(tokens, gate_up_weight[rank_dimension], preferred_element_type=single_float)
        preactivation = preactivation + adapter_scale * jnp.dot(lower_projection, gate_up_output_factor[rank_dimension].astype(single_float), precision=upper_projection)
        pres.append(preactivation)
    gate, upper = pres[0], pres[1]
    hidden_state = (jax.nn.silu(gate) * upper).astype(jnp.bfloat16)
    lower_down_projection = jnp.dot(hidden_state, down_input_factor, preferred_element_type=single_float)
    output = jnp.dot(hidden_state, down_weight, preferred_element_type=single_float)
    output = output + adapter_scale * jnp.dot(lower_down_projection, down_output_factor.astype(single_float), precision=upper_projection)
    output = output.astype(jnp.bfloat16)
    backward_down_rows = jnp.dot(cotangent, down_output_factor.T, preferred_element_type=single_float).astype(jnp.bfloat16)
    hidden_state_gradient = jnp.dot(cotangent, down_weight.T, preferred_element_type=single_float)
    hidden_state_gradient = hidden_state_gradient + adapter_scale * jnp.dot(backward_down_rows, down_input_factor.T, preferred_element_type=single_float)
    down_input_factor_gradient = adapter_scale * scale_factor * jnp.dot(hidden_state.T, backward_down_rows, preferred_element_type=single_float)
    down_output_factor_gradient = adapter_scale * scale_factor * jnp.dot(lower_down_projection.T, cotangent.astype(single_float), precision=upper_projection)
    sigma = jax.nn.sigmoid(gate)
    gate_back = (hidden_state_gradient * upper * sigma * (1.0 + gate * (1.0 - sigma))).astype(jnp.bfloat16)
    up_back = (hidden_state_gradient * gate * sigma).astype(jnp.bfloat16)
    backward_results = [gate_back, up_back]
    output_factor_gradient = []
    input_factor_gradient = []
    input_total_sum = jnp.zeros(tokens.shape, single_float)
    for rank_dimension in range(2):
        output_factor_gradient.append(adapter_scale * scale_factor * jnp.dot(lower_results[rank_dimension].T, backward_results[rank_dimension].astype(single_float), precision=upper_projection))
        backward_lower_rows = jnp.dot(backward_results[rank_dimension], gate_up_output_factor[rank_dimension].T, preferred_element_type=single_float).astype(jnp.bfloat16)
        input_factor_gradient.append(adapter_scale * scale_factor * jnp.dot(tokens.T, backward_lower_rows, preferred_element_type=single_float))
        input_total_sum = input_total_sum + jnp.dot(backward_results[rank_dimension], gate_up_weight[rank_dimension].T, preferred_element_type=single_float)
        input_total_sum = input_total_sum + adapter_scale * jnp.dot(backward_lower_rows, gate_up_input_factor[rank_dimension].T, preferred_element_type=single_float)
    input_grad = input_total_sum.astype(jnp.bfloat16)
    return (output, input_grad, jnp.stack(input_factor_gradient), jnp.stack(output_factor_gradient), down_input_factor_gradient, down_output_factor_gradient)
```

```python
import jax
import jax.numpy as jnp
from jax import lax
from jax.sharding import Mesh
from jax.sharding import PartitionSpec as P

F32 = jnp.float32
BF16 = jnp.bfloat16
adapter_scale = 2.0
CUT = 896


def shifted(x, axis, by):
    n = lax.axis_size(axis)
    return lax.ppermute(x, axis, [(i, (i + by) % n) for i in range(n)])


def other_core(x):
    return lax.ppermute(x, "dp", [(i, i ^ 1) for i in range(lax.axis_size("dp"))])


def to_chip(x, by):
    n = lax.axis_size("dp")
    return lax.ppermute(x, "dp", [(i, (i + 2 * by) % n) for i in range(n)])


def dot(a, b, dims=((1,), (0,))):
    return lax.dot_general(a, b, (dims, ((), ())), preferred_element_type=F32)


def gather_direct(x, axis):
    return jnp.stack([x, shifted(x, axis, -1), shifted(x, axis, 2), shifted(x, axis, 1)])


def gather_ring(x, axis):
    after, before = shifted(x, axis, -1), shifted(x, axis, 1)
    h = x.shape[-1] // 256 * 128
    a = shifted(before[..., :h], axis, 1)
    b = shifted(after[..., h:], axis, -1)
    return jnp.stack([x, after, jnp.concatenate([a, b], -1), before])


def gathered(x, first, second):
    g = gather_ring(gather_direct(x, first), second)
    if first == "y":
        g = g.transpose(1, 0, 2, 3)
    return g.reshape(256, x.shape[-1])


def sum_direct(x, axis):
    return (
        x[0].astype(F32)
        + shifted(x[1], axis, 1).astype(F32)
        + shifted(x[2], axis, 2).astype(F32)
        + shifted(x[3], axis, -1).astype(F32)
    )


def sum_ring(x, axis):
    h = x.shape[-1] // 256 * 128
    a = shifted(x[2][..., :h], axis, 1)
    b = shifted(x[2][..., h:], axis, -1)
    up = jnp.concatenate(
        [(x[1][..., :h].astype(F32) + a.astype(F32)).astype(BF16), x[1][..., h:]], -1
    )
    down = jnp.concatenate(
        [x[3][..., :h], (x[3][..., h:].astype(F32) + b.astype(F32)).astype(BF16)], -1
    )
    return x[0].astype(F32) + shifted(up, axis, 1).astype(F32) + shifted(down, axis, -1).astype(F32)


def scattered_sum(x, first, second):
    x = x.reshape(4, 4, 16, x.shape[-1])
    if first == "z":
        x = x.transpose(1, 0, 2, 3)
    return sum_direct(sum_direct(x, first).astype(BF16), second)


def per_device(
    tokens,
    gate_up_weight,
    down_weight,
    gate_up_input_factor,
    gate_up_output_factor,
    down_input_factor,
    down_output_factor,
    cotangent,
):
    scale = adapter_scale * 256 ** (-0.5)
    dp = lax.axis_index("dp")
    chip, core = dp // 2, dp % 2
    y, z = lax.axis_index("y"), lax.axis_index("z")

    mine = jnp.concatenate([tokens, cotangent], 1)
    pair = jnp.concatenate([mine, other_core(mine)], 0)
    near = jnp.concatenate([pair, to_chip(pair, -1), to_chip(pair, 2), to_chip(pair, 1)], 0)

    n = jnp.arange(256, dtype=jnp.int32)
    token_of_row = 64 * ((y + n // 64) % 4) + 16 * ((z + n // 16 % 4) % 4) + n % 16
    token_of_near = 64 * ((chip + n // 64) % 4) + 32 * (core ^ (n // 32 % 2)) + n % 32
    turn = (token_of_row[:, None] == token_of_near[None, :]).astype(BF16)
    rows = dot(turn, near).astype(BF16)
    x, c = rows[:, :512], rows[:, 512:]

    wg, wu = gate_up_weight[0], gate_up_weight[1]
    a_both = jnp.concatenate([gate_up_input_factor[0], gate_up_input_factor[1]], 1)
    low_part = dot(x, a_both)
    back_down_part = dot(c, down_output_factor, ((1,), (1,)))
    part_a = jnp.concatenate(
        [
            low_part,
            back_down_part,
            jnp.zeros((256, 64), F32),
            dot(x, wg[:, :CUT]),
            dot(x, wu[:, :CUT]),
            dot(c, down_weight[:CUT], ((1,), (1,))),
        ],
        1,
    ).astype(BF16)
    part_b = jnp.concatenate(
        [
            dot(x, wg[:, CUT:]),
            dot(x, wu[:, CUT:]),
            dot(c, down_weight[CUT:], ((1,), (1,))),
        ],
        1,
    ).astype(BF16)
    sum_a = scattered_sum(part_a, "y", "z")
    sum_b = scattered_sum(part_b, "z", "y")
    low, back_down = sum_a[:, :128], sum_a[:, 128:192].astype(BF16)

    def middle(gate, up, back, cols):
        bg = gate_up_output_factor[0][:, cols].astype(F32)
        bu = gate_up_output_factor[1][:, cols].astype(F32)
        gate = gate + adapter_scale * dot(low[:, :64], bg)
        up = up + adapter_scale * dot(low[:, 64:], bu)
        back = back + adapter_scale * dot(back_down, down_input_factor[cols], ((1,), (1,)))
        s = jax.nn.sigmoid(gate)
        hidden = (gate * s * up).astype(BF16)
        gate_back = (back * up * s * (1.0 + gate * (1.0 - s))).astype(BF16)
        up_back = (back * gate * s).astype(BF16)
        return hidden, gate_back, up_back

    w = CUT
    parts_a = middle(
        sum_a[:, 256 : 256 + w], sum_a[:, 256 + w : 256 + 2 * w], sum_a[:, 256 + 2 * w :], slice(0, w)
    )
    v = 1920 - CUT
    parts_b = middle(sum_b[:, :v], sum_b[:, v : 2 * v], sum_b[:, 2 * v :], slice(w, 1920))
    all_a = gathered(
        jnp.concatenate(
            [low.astype(BF16), back_down, jnp.zeros((16, 64), BF16), *parts_a], 1
        ),
        "z",
        "y",
    )
    all_b = gathered(jnp.concatenate(parts_b, 1), "y", "z")
    low_all, back_down_all = all_a[:, :128], all_a[:, 128:192]
    hidden_a, gate_a, up_a = (all_a[:, 256 + i * w : 256 + (i + 1) * w] for i in range(3))
    hidden_b, gate_b, up_b = (all_b[:, i * v : (i + 1) * v] for i in range(3))

    t = ((1,), (1,))
    bo = gate_up_output_factor
    back_low_part = jnp.concatenate(
        [
            dot(gate_a, bo[0][:, :w], t) + dot(gate_b, bo[0][:, w:], t),
            dot(up_a, bo[1][:, :w], t) + dot(up_b, bo[1][:, w:], t),
        ],
        1,
    )
    low_down_part = dot(hidden_a, down_input_factor[:w]) + dot(hidden_b, down_input_factor[w:])
    out_part = (
        dot(hidden_a, down_weight[:w])
        + dot(hidden_b, down_weight[w:])
        + adapter_scale * dot(low_down_part, down_output_factor.astype(F32))
    )
    grad_part = (
        dot(gate_a, wg[:, :w], t)
        + dot(gate_b, wg[:, w:], t)
        + dot(up_a, wu[:, :w], t)
        + dot(up_b, wu[:, w:], t)
    )
    sums = jnp.concatenate(
        [back_low_part, low_down_part, jnp.zeros((256, 64), F32), out_part, grad_part], 1
    ).astype(BF16)
    sums = dot(turn, sums, ((0,), (0,))).astype(BF16).reshape(4, 2, 32, 1280)
    sums = (sums[:, 0].astype(F32) + other_core(sums[:, 1]).astype(F32)).astype(BF16)
    small, large = sums[..., :256], sums[..., 256:]
    small_sum, large_sum = small.astype(F32), large[0].astype(F32)
    for k in (1, 3, 2):
        sent = jnp.concatenate([large[k]] + [small[j] for j in range(4)], 1)
        got = to_chip(sent, k)
        large_sum = large_sum + got[:, :1024].astype(F32)
        theirs = [got[:, 1024 + 256 * j : 1280 + 256 * j] for j in range(4)]
        small_sum = small_sum + jnp.stack([theirs[(j + k) % 4] for j in range(4)]).astype(F32)
    small_sum = small_sum.astype(BF16)
    small_all = jnp.stack([small_sum, other_core(small_sum)], 1).reshape(256, 256)
    back_low_all, low_down_all = small_all[:, :128], small_all[:, 128:192]

    output = large_sum[:, :512].astype(BF16)
    back_low = small_sum[0][:, :128]
    input_grad = (large_sum[:, 512:] + adapter_scale * dot(back_low, a_both, t)).astype(BF16)
    lower = scale * dot(near[:, :512], back_low_all, ((0,), (0,)))
    grad_gate_up_lower = jnp.stack([lower[:, :64], lower[:, 64:]])
    down_output_factor_gradient = scale * dot(low_down_all, near[:, 512:], ((0,), (0,)))
    o = ((0,), (0,))
    gate_up_output_factor_gradient = scale * jnp.stack(
        [
            jnp.concatenate([dot(low_all[:, :64], gate_a, o), dot(low_all[:, :64], gate_b, o)], 1),
            jnp.concatenate([dot(low_all[:, 64:], up_a, o), dot(low_all[:, 64:], up_b, o)], 1),
        ]
    )
    down_input_factor_gradient = scale * jnp.concatenate(
        [dot(hidden_a, back_down_all, o), dot(hidden_b, back_down_all, o)], 0
    )
    return (
        output,
        input_grad,
        grad_gate_up_lower,
        gate_up_output_factor_gradient,
        down_input_factor_gradient,
        down_output_factor_gradient,
    )


def solution(mesh):
    torus = Mesh(mesh.devices.reshape(mesh.shape["dp"], 4, 4), ("dp", "y", "z"))
    mp = ("y", "z")
    in_specs = (
        P("dp", mp),
        P(None, mp, "dp"),
        P("dp", mp),
        P(None, mp, None),
        P(None, None, "dp"),
        P("dp", None),
        P(None, mp),
        P("dp", mp),
    )
    out_specs = (
        P("dp", mp),
        P("dp", mp),
        P(None, mp, None),
        P(None, None, "dp"),
        P("dp", None),
        P(None, mp),
    )
    return jax.shard_map(
        per_device, mesh=torus, in_specs=in_specs, out_specs=out_specs, check_vma=False
    )
```

```python
import jax
import jax.numpy as jnp
from jax import lax
from jax.experimental import pallas as pl
from jax.experimental.pallas import tpu as pltpu
from jax.sharding import Mesh
from jax.sharding import PartitionSpec as P

F32 = jnp.float32
BF16 = jnp.bfloat16
adapter_scale = 2.0
CUT = 896


def other_core(x):
    return lax.ppermute(x, "dp", [(i, i ^ 1) for i in range(lax.axis_size("dp"))])


def to_chip(x, by):
    n = lax.axis_size("dp")
    return lax.ppermute(x, "dp", [(i, (i + 2 * by) % n) for i in range(n)])


def dot(a, b, dims=((1,), (0,))):
    return lax.dot_general(a, b, (dims, ((), ())), preferred_element_type=F32)


def along(x, stage, by):
    pairs = []
    for dp in range(8):
        for y in range(4):
            for z in range(4):
                if (dp + stage) % 2 == 0:
                    there = (y + by) % 4 * 4 + z
                else:
                    there = y * 4 + (z + by) % 4
                pairs.append((dp * 16 + y * 4 + z, dp * 16 + there))
    return lax.ppermute(x, ("dp", "y", "z"), pairs)


def sum_direct(x, stage):
    return (
        x[0].astype(F32)
        + along(x[1], stage, 1).astype(F32)
        + along(x[3], stage, -1).astype(F32)
        + along(x[2], stage, 2).astype(F32)
    )


def scattered_sum(x):
    x = sum_direct(x, 0).astype(BF16)
    return sum_direct(x.reshape(4, 16, x.shape[-1]), 1)


def gather_direct(x, stage):
    after, before = along(x, stage, -1), along(x, stage, 1)
    return jnp.stack([x, after, along(x, stage, 2), before])


def gather_ring(x, stage):
    after, before = along(x, stage, -1), along(x, stage, 1)
    h = x.shape[-1] // 256 * 128
    a = along(before[..., :h], stage, 1)
    b = along(after[..., h:], stage, -1)
    return jnp.stack([x, after, jnp.concatenate([a, b], -1), before])


def gathered(x):
    return gather_direct(gather_direct(x, 1), 0).reshape(256, x.shape[-1])


def whole(n):
    return [pl.BlockSpec(memory_space=pltpu.VMEM)] * n


def in_vmem(shape, dtype):
    return pltpu.VMEM(shape, dtype)


T = ((1,), (1,))


def tiles(lo, hi, step=384):
    return [(a, min(a + step, hi)) for a in range(lo, hi, step)]


def store_blocks(outs, at, value):
    value = value.astype(BF16)
    for k in range(4):
        outs[k][:, at : at + value.shape[1]] = value[64 * k : 64 * k + 64]


def first_kernel(turn, near, wgu, wd, a_both, dof, rows, *outs):
    rows[...] = dot(turn[...], near[...]).astype(BF16)
    x, c = rows[:, :512], rows[:, 512:]
    store_blocks(outs, 0, dot(x, a_both[...]))
    store_blocks(outs, 128, dot(c, dof[...], T))
    for k in range(2):
        for lo, hi in tiles(0, CUT):
            store_blocks(outs, 256 + k * CUT + lo, dot(x, wgu[k, :, lo:hi]))
    for lo, hi in tiles(0, CUT):
        store_blocks(outs, 256 + 2 * CUT + lo, dot(c, wd[lo:hi, :], T))


def first_half(turn, near, wgu, wd, a_both, dof):
    block = in_vmem((64, 256 + 3 * CUT), BF16)
    return pl.pallas_call(
        first_kernel,
        out_shape=[in_vmem((256, 1024), BF16)] + [block] * 4,
        in_specs=whole(6),
        out_specs=whole(5),
        compiler_params=pltpu.CompilerParams(vmem_limit_bytes=12 * 2**20),
        cost_estimate=pl.CostEstimate(flops=10**9, bytes_accessed=10**6, transcendentals=0),
    )(turn, near, wgu, wd, a_both, dof)


def second_kernel(rows, wgu, wd, *outs):
    x, c = rows[:, :512], rows[:, 512:]
    n = 1920 - CUT
    for k in range(2):
        for lo, hi in tiles(CUT, 1920):
            store_blocks(outs, k * n + lo - CUT, dot(x, wgu[k, :, lo:hi]))
    for lo, hi in tiles(CUT, 1920):
        store_blocks(outs, 2 * n + lo - CUT, dot(c, wd[lo:hi, :], T))


def second_half(rows, wgu, wd):
    block = in_vmem((64, 3 * (1920 - CUT)), BF16)
    return pl.pallas_call(
        second_kernel,
        out_shape=[block] * 4,
        in_specs=whole(3),
        out_specs=whole(4),
        compiler_params=pltpu.CompilerParams(vmem_limit_bytes=12 * 2**20),
        cost_estimate=pl.CostEstimate(flops=10**9, bytes_accessed=10**6, transcendentals=0),
    )(rows, wgu, wd)


def back_products(g, at, lo, hi, wgu, wd, bo, dif):
    w = hi - lo
    hidden, gate, up = (g[:, at + k * w : at + (k + 1) * w] for k in range(3))
    return (
        dot(gate, bo[0, :, lo:hi], T),
        dot(up, bo[1, :, lo:hi], T),
        dot(hidden, dif[lo:hi, :]),
        dot(hidden, wd[lo:hi, :]),
        dot(gate, wgu[0, :, lo:hi], T) + dot(up, wgu[1, :, lo:hi], T),
    )


def third_kernel(g, wgu, wd, bo, dif, small, out, grad):
    bl0, bl1, ld, o, d = back_products(g, 256, 0, CUT, wgu, wd, bo, dif)
    small[:, :64] = bl0
    small[:, 64:128] = bl1
    small[:, 128:192] = ld
    out[...] = o
    grad[...] = d


def third_half(g, wgu, wd, bo, dif):
    return pl.pallas_call(
        third_kernel,
        out_shape=[
            in_vmem((256, 256), F32),
            in_vmem((256, 512), F32),
            in_vmem((256, 512), F32),
        ],
        in_specs=whole(5),
        out_specs=whole(3),
        compiler_params=pltpu.CompilerParams(vmem_limit_bytes=12 * 2**20),
        cost_estimate=pl.CostEstimate(flops=10**9, bytes_accessed=10**6, transcendentals=0),
    )(g, wgu, wd, bo, dif)


def fourth_kernel(g, wgu, wd, bo, dif, dof, turn, small, out, grad, mine, theirs):
    bl0, bl1, ld, o, d = back_products(g, 0, CUT, 1920, wgu, wd, bo, dif)
    low_down = small[:, 128:192] + ld
    o = o + out[...] + adapter_scale * dot(low_down.astype(BF16), dof[...])

    def turned(value):
        value = dot(turn[...], value.astype(BF16), ((0,), (0,)))
        return value

    def put(value, at):
        value = turned(value)
        for k in range(4):
            mine[k, :, at : at + value.shape[1]] = value[64 * k : 64 * k + 32].astype(BF16)
            theirs[k, :, at : at + value.shape[1]] = value[64 * k + 32 : 64 * k + 64].astype(BF16)

    put(small[:, :64] + bl0, 0)
    put(small[:, 64:128] + bl1, 64)
    put(low_down, 128)
    put(jnp.zeros((256, 64), F32), 192)
    put(o, 256)
    put(d + grad[...], 768)


def fourth_half(g, wgu, wd, bo, dif, dof, turn, small, out, grad):
    block = in_vmem((4, 32, 1280), BF16)
    return pl.pallas_call(
        fourth_kernel,
        out_shape=[block, block],
        in_specs=whole(10),
        out_specs=whole(2),
        compiler_params=pltpu.CompilerParams(vmem_limit_bytes=12 * 2**20),
        cost_estimate=pl.CostEstimate(flops=10**9, bytes_accessed=10**6, transcendentals=0),
    )(g, wgu, wd, bo, dif, dof, turn, small, out, grad)


def per_device(
    tokens,
    gate_up_weight,
    down_weight,
    gate_up_input_factor,
    gate_up_output_factor,
    down_input_factor,
    down_output_factor,
    cotangent,
):
    scale = adapter_scale * 256 ** (-0.5)
    dp = lax.axis_index("dp")
    chip, core = dp // 2, dp % 2
    y, z = lax.axis_index("y"), lax.axis_index("z")

    mine = jnp.concatenate([tokens, cotangent], 1)
    pair = jnp.concatenate([mine, other_core(mine)], 0)
    near = jnp.concatenate([pair, to_chip(pair, -1), to_chip(pair, 2), to_chip(pair, 1)], 0)

    n = jnp.arange(256, dtype=jnp.int32)
    first, second = n // 64, n // 16 % 4
    y_by, z_by = jnp.where(core == 0, first, second), jnp.where(core == 0, second, first)
    token_of_row = 64 * ((y + y_by) % 4) + 16 * ((z + z_by) % 4) + n % 16
    token_of_near = 64 * ((chip + n // 64) % 4) + 32 * (core ^ (n // 32 % 2)) + n % 32
    turn = (token_of_row[:, None] == token_of_near[None, :]).astype(BF16)
    wgu, wd, bo, dif = gate_up_weight, down_weight, gate_up_output_factor, down_input_factor
    dof = down_output_factor
    a_both = jnp.concatenate([gate_up_input_factor[0], gate_up_input_factor[1]], 1)
    rows, *part_a = first_half(turn, near, wgu, wd, a_both, dof)
    part_b = second_half(rows, wgu, wd)
    sum_a = scattered_sum(part_a)
    sum_b = scattered_sum(part_b)
    low, back_down = sum_a[:, :128], sum_a[:, 128:192].astype(BF16)

    def middle(gate, up, back, cols):
        bg = bo[0][:, cols].astype(F32)
        bu = bo[1][:, cols].astype(F32)
        gate = gate + adapter_scale * dot(low[:, :64], bg)
        up = up + adapter_scale * dot(low[:, 64:], bu)
        back = back + adapter_scale * dot(back_down, dif[cols], T)
        s = jax.nn.sigmoid(gate)
        hidden = (gate * s * up).astype(BF16)
        gate_back = (back * up * s * (1.0 + gate * (1.0 - s))).astype(BF16)
        up_back = (back * gate * s).astype(BF16)
        return hidden, gate_back, up_back

    w = CUT
    parts_a = middle(
        sum_a[:, 256 : 256 + w], sum_a[:, 256 + w : 256 + 2 * w], sum_a[:, 256 + 2 * w :], slice(0, w)
    )
    v = 1920 - CUT
    parts_b = middle(sum_b[:, :v], sum_b[:, v : 2 * v], sum_b[:, 2 * v :], slice(w, 1920))
    all_a = gathered(
        jnp.concatenate(
            [low.astype(BF16), back_down, jnp.zeros((16, 64), BF16), *parts_a], 1
        ),
    )
    all_b = gathered(jnp.concatenate(parts_b, 1))
    low_all, back_down_all = all_a[:, :128], all_a[:, 128:192]
    hidden_a, gate_a, up_a = (all_a[:, 256 + i * w : 256 + (i + 1) * w] for i in range(3))
    hidden_b, gate_b, up_b = (all_b[:, i * v : (i + 1) * v] for i in range(3))

    t = T
    halves = third_half(all_a, wgu, wd, bo, dif)
    sums, sent = fourth_half(all_b, wgu, wd, bo, dif, dof, turn, *halves)
    arrived = other_core(sent)
    low_all, back_down_all, hidden_a, hidden_b, gate_a, gate_b, up_a, up_b, arrived = (
        lax.optimization_barrier(
            (low_all, back_down_all, hidden_a, hidden_b, gate_a, gate_b, up_a, up_b, arrived)
        )
    )
    sums = (sums.astype(F32) + arrived.astype(F32)).astype(BF16)
    small, large = sums[..., :256], sums[..., 256:]
    small_sum, large_sum = small.astype(F32), large[0].astype(F32)
    for k in (1, 3, 2):
        sent = jnp.concatenate([large[k]] + [small[j] for j in range(4)], 1)
        got = to_chip(sent, k)
        large_sum = large_sum + got[:, :1024].astype(F32)
        theirs = [got[:, 1024 + 256 * j : 1280 + 256 * j] for j in range(4)]
        small_sum = small_sum + jnp.stack([theirs[(j + k) % 4] for j in range(4)]).astype(F32)
    small_sum = small_sum.astype(BF16)
    small_all = jnp.stack([small_sum, other_core(small_sum)], 1).reshape(256, 256)
    back_low_all, low_down_all = small_all[:, :128], small_all[:, 128:192]

    output = large_sum[:, :512].astype(BF16)
    back_low = small_sum[0][:, :128]
    input_grad = (large_sum[:, 512:] + adapter_scale * dot(back_low, a_both, t)).astype(BF16)
    lower = scale * dot(near[:, :512], back_low_all, ((0,), (0,)))
    grad_gate_up_lower = jnp.stack([lower[:, :64], lower[:, 64:]])
    down_output_factor_gradient = scale * dot(low_down_all, near[:, 512:], ((0,), (0,)))
    o = ((0,), (0,))
    gate_up_output_factor_gradient = scale * jnp.stack(
        [
            jnp.concatenate([dot(low_all[:, :64], gate_a, o), dot(low_all[:, :64], gate_b, o)], 1),
            jnp.concatenate([dot(low_all[:, 64:], up_a, o), dot(low_all[:, 64:], up_b, o)], 1),
        ]
    )
    down_input_factor_gradient = scale * jnp.concatenate(
        [dot(hidden_a, back_down_all, o), dot(hidden_b, back_down_all, o)], 0
    )
    return (
        output,
        input_grad,
        grad_gate_up_lower,
        gate_up_output_factor_gradient,
        down_input_factor_gradient,
        down_output_factor_gradient,
    )


def solution(mesh):
    torus = Mesh(mesh.devices.reshape(mesh.shape["dp"], 4, 4), ("dp", "y", "z"))
    mp = ("y", "z")
    in_specs = (
        P("dp", mp),
        P(None, mp, "dp"),
        P("dp", mp),
        P(None, mp, None),
        P(None, None, "dp"),
        P("dp", None),
        P(None, mp),
        P("dp", mp),
    )
    out_specs = (
        P("dp", mp),
        P("dp", mp),
        P(None, mp, None),
        P(None, None, "dp"),
        P("dp", None),
        P(None, mp),
    )
    return jax.shard_map(
        per_device, mesh=torus, in_specs=in_specs, out_specs=out_specs, check_vma=False
    )
```

```python
import jax
import jax.numpy as jnp
from jax import lax
from jax.experimental import pallas as pl
from jax.experimental.pallas import tpu as pltpu
from jax.sharding import Mesh
from jax.sharding import PartitionSpec as P

F32 = jnp.float32
BF16 = jnp.bfloat16
adapter_scale = 2.0
CUT = 896


def other_core(x):
    return lax.ppermute(x, "dp", [(i, i ^ 1) for i in range(lax.axis_size("dp"))])


def to_chip(x, by):
    n = lax.axis_size("dp")
    return lax.ppermute(x, "dp", [(i, (i + 2 * by) % n) for i in range(n)])


def dot(a, b, dims=((1,), (0,))):
    return lax.dot_general(a, b, (dims, ((), ())), preferred_element_type=F32)


def along(x, stage, by):
    pairs = []
    for dp in range(8):
        for y in range(4):
            for z in range(4):
                if (dp + stage) % 2 == 0:
                    there = (y + by) % 4 * 4 + z
                else:
                    there = y * 4 + (z + by) % 4
                pairs.append((dp * 16 + y * 4 + z, dp * 16 + there))
    return lax.ppermute(x, ("dp", "y", "z"), pairs)


def exchanged(blocks, stage):
    return [
        blocks[0],
        along(blocks[1], stage, 1),
        along(blocks[3], stage, -1),
        along(blocks[2], stage, 2),
    ]


def collected(block, stage):
    return [block, along(block, stage, -1), along(block, stage, 2), along(block, stage, 1)]


def whole(n):
    return [pl.BlockSpec(memory_space=pltpu.VMEM)] * n


def in_vmem(shape, dtype):
    return pltpu.VMEM(shape, dtype)


T = ((1,), (1,))


def tiles(lo, hi, step=384):
    return [(a, min(a + step, hi)) for a in range(lo, hi, step)]


def store_blocks(outs, at, value):
    value = value.astype(BF16)
    for k in range(4):
        outs[k][:, at : at + value.shape[1]] = value[64 * k : 64 * k + 64]


def first_kernel(turn, near, wgu, wd, a_both, dof, rows, *outs):
    rows[...] = dot(turn[...], near[...]).astype(BF16)
    x, c = rows[:, :512], rows[:, 512:]
    store_blocks(outs, 0, dot(x, a_both[...]))
    store_blocks(outs, 128, dot(c, dof[...], T))
    store_blocks(outs, 192, jnp.zeros((256, 64), F32))
    for k in range(2):
        for lo, hi in tiles(0, CUT):
            store_blocks(outs, 256 + k * CUT + lo, dot(x, wgu[k, :, lo:hi]))
    for lo, hi in tiles(0, CUT):
        store_blocks(outs, 256 + 2 * CUT + lo, dot(c, wd[lo:hi, :], T))


def first_half(turn, near, wgu, wd, a_both, dof):
    block = in_vmem((64, 256 + 3 * CUT), BF16)
    return pl.pallas_call(
        first_kernel,
        out_shape=[in_vmem((256, 1024), BF16)] + [block] * 4,
        in_specs=whole(6),
        out_specs=whole(5),
        compiler_params=pltpu.CompilerParams(vmem_limit_bytes=12 * 2**20),
        cost_estimate=pl.CostEstimate(flops=10**9, bytes_accessed=10**6, transcendentals=0),
    )(turn, near, wgu, wd, a_both, dof)


def second_kernel(rows, wgu, wd, *outs):
    x, c = rows[:, :512], rows[:, 512:]
    n = 1920 - CUT
    for k in range(2):
        for lo, hi in tiles(CUT, 1920):
            store_blocks(outs, k * n + lo - CUT, dot(x, wgu[k, :, lo:hi]))
    for lo, hi in tiles(CUT, 1920):
        store_blocks(outs, 2 * n + lo - CUT, dot(c, wd[lo:hi, :], T))


def second_half(rows, wgu, wd):
    block = in_vmem((64, 3 * (1920 - CUT)), BF16)
    return pl.pallas_call(
        second_kernel,
        out_shape=[block] * 4,
        in_specs=whole(3),
        out_specs=whole(4),
        compiler_params=pltpu.CompilerParams(vmem_limit_bytes=12 * 2**20),
        cost_estimate=pl.CostEstimate(flops=10**9, bytes_accessed=10**6, transcendentals=0),
    )(rows, wgu, wd)


def params(mib=12):
    return pltpu.CompilerParams(vmem_limit_bytes=mib * 2**20)


def cost(flops):
    return pl.CostEstimate(flops=flops, bytes_accessed=10**6, transcendentals=0)


def total(refs):
    return (
        refs[0][...].astype(F32)
        + refs[1][...].astype(F32)
        + refs[2][...].astype(F32)
        + refs[3][...].astype(F32)
    )


def sum_kernel(*refs):
    value = total(refs[:4]).astype(BF16)
    for k in range(4):
        refs[4 + k][...] = value[16 * k : 16 * k + 16]


def summed(blocks):
    out = in_vmem((16, blocks[0].shape[1]), BF16)
    return pl.pallas_call(
        sum_kernel,
        out_shape=[out] * 4,
        in_specs=whole(4),
        out_specs=whole(4),
        compiler_params=params(),
        cost_estimate=cost(10**7),
    )(*blocks)


def middle(low, back_down, value, at, lo, hi, bo, dif, out):
    w = hi - lo
    low = low.astype(BF16)
    gate = value[:, at : at + w] + adapter_scale * dot(low[:, :64], bo[0, :, lo:hi])
    up = value[:, at + w : at + 2 * w] + adapter_scale * dot(low[:, 64:], bo[1, :, lo:hi])
    back = value[:, at + 2 * w :] + adapter_scale * dot(back_down, dif[:, lo:hi])
    s = jax.nn.sigmoid(gate)
    out[:, at : at + w] = (gate * s * up).astype(BF16)
    out[:, at + w : at + 2 * w] = (back * up * s * (1.0 + gate * (1.0 - s))).astype(BF16)
    out[:, at + 2 * w :] = (back * gate * s).astype(BF16)


def middle_first_kernel(a, b, c, d, bo, dif, out):
    value = total((a, b, c, d))
    small = value[:, :256].astype(BF16)
    out[:, :256] = small
    middle(value[:, :128], small[:, 128:192], value, 256, 0, CUT, bo, dif, out)


def middle_second_kernel(a, b, c, d, first, bo, dif, out):
    value = total((a, b, c, d))
    middle(first[:, :128], first[:, 128:192], value, 0, CUT, 1920, bo, dif, out)


def middles(blocks, bo, dif, first=None):
    more = [] if first is None else [first]
    return pl.pallas_call(
        middle_first_kernel if first is None else middle_second_kernel,
        out_shape=in_vmem(blocks[0].shape, BF16),
        in_specs=whole(6 + len(more)),
        out_specs=whole(1)[0],
        compiler_params=params(),
        cost_estimate=cost(10**8),
    )(*blocks, *more, bo, dif)


def stack_kernel(a, b, c, d, out):
    for k, ref in enumerate((a, b, c, d)):
        out[16 * k : 16 * k + 16] = ref[...]


def stacked(blocks):
    return pl.pallas_call(
        stack_kernel,
        out_shape=in_vmem((64, blocks[0].shape[1]), BF16),
        in_specs=whole(4),
        out_specs=whole(1)[0],
        compiler_params=params(),
        cost_estimate=cost(10**7),
    )(*blocks)


def joined(refs, lo, hi):
    return jnp.concatenate([ref[:, lo:hi] for ref in refs], 0)


def factor_kernel(*refs):
    a, b, bo_grad, dif_grad = refs[:4], refs[4:8], refs[8], refs[9]
    n = ((0,), (0,))
    scale = adapter_scale * 256 ** (-0.5)
    small = joined(a, 0, 256)
    low, back_down = small[:, :128], small[:, 128:192]
    for part, at, lo, hi in ((a, 256, 0, CUT), (b, 0, CUT, 1920)):
        w = hi - lo
        dif_grad[lo:hi, :] = scale * dot(joined(part, at, at + w), back_down, n)
        for k in range(2):
            g = joined(part, at + (k + 1) * w, at + (k + 2) * w)
            bo_grad[k, :, lo:hi] = scale * dot(low[:, 64 * k : 64 * k + 64], g, n)


def factor_gradients(a, b):
    return pl.pallas_call(
        factor_kernel,
        out_shape=[
            jax.ShapeDtypeStruct((2, 64, 1920), F32),
            jax.ShapeDtypeStruct((1920, 64), F32),
        ],
        in_specs=whole(8),
        out_specs=whole(2),
        compiler_params=params(16),
        cost_estimate=cost(4 * 10**9),
    )(*a, *b)


def back_products(g, at, lo, hi, wgu, wd, bo, dif):
    w = hi - lo
    hidden, gate, up = (joined(g, at + k * w, at + (k + 1) * w) for k in range(3))
    return (
        dot(gate, bo[0, :, lo:hi], T),
        dot(up, bo[1, :, lo:hi], T),
        dot(hidden, dif[:, lo:hi], T),
        dot(hidden, wd[lo:hi, :]),
        dot(gate, wgu[0, :, lo:hi], T) + dot(up, wgu[1, :, lo:hi], T),
    )


def third_kernel(a, b, c, d, wgu, wd, bo, dif, small, out, grad):
    bl0, bl1, ld, o, g = back_products((a, b, c, d), 256, 0, CUT, wgu, wd, bo, dif)
    small[:, :64] = bl0
    small[:, 64:128] = bl1
    small[:, 128:192] = ld
    out[...] = o
    grad[...] = g


def third_half(g, wgu, wd, bo, dif):
    return pl.pallas_call(
        third_kernel,
        out_shape=[
            in_vmem((256, 256), F32),
            in_vmem((256, 512), F32),
            in_vmem((256, 512), F32),
        ],
        in_specs=whole(8),
        out_specs=whole(3),
        compiler_params=params(),
        cost_estimate=cost(10**9),
    )(*g, wgu, wd, bo, dif)


def fourth_kernel(a, b, c, d, wgu, wd, bo, dif, dof, turn, small, out, grad, mine, theirs):
    bl0, bl1, ld, o, g = back_products((a, b, c, d), 0, CUT, 1920, wgu, wd, bo, dif)
    low_down = small[:, 128:192] + ld
    o = o + out[...] + adapter_scale * dot(low_down.astype(BF16), dof[...])

    def put(value, at):
        value = dot(turn[...], value.astype(BF16), ((0,), (0,)))
        for k in range(4):
            mine[k, :, at : at + value.shape[1]] = value[64 * k : 64 * k + 32].astype(BF16)
            theirs[k, :, at : at + value.shape[1]] = value[64 * k + 32 : 64 * k + 64].astype(BF16)

    put(small[:, :64] + bl0, 0)
    put(small[:, 64:128] + bl1, 64)
    put(low_down, 128)
    put(jnp.zeros((256, 64), F32), 192)
    put(o, 256)
    put(g + grad[...], 768)


def fourth_half(g, wgu, wd, bo, dif, dof, turn, small, out, grad):
    block = in_vmem((4, 32, 1280), BF16)
    return pl.pallas_call(
        fourth_kernel,
        out_shape=[block, block],
        in_specs=whole(13),
        out_specs=whole(2),
        compiler_params=params(),
        cost_estimate=cost(10**9),
    )(*g, wgu, wd, bo, dif, dof, turn, small, out, grad)


def per_device(
    tokens,
    gate_up_weight,
    down_weight,
    gate_up_input_factor,
    gate_up_output_factor,
    down_input_factor,
    down_output_factor,
    cotangent,
):
    scale = adapter_scale * 256 ** (-0.5)
    dp = lax.axis_index("dp")
    chip, core = dp // 2, dp % 2
    y, z = lax.axis_index("y"), lax.axis_index("z")

    mine = jnp.concatenate([tokens, cotangent], 1)
    pair = jnp.concatenate([mine, other_core(mine)], 0)
    near = jnp.concatenate([pair, to_chip(pair, -1), to_chip(pair, 2), to_chip(pair, 1)], 0)

    n = jnp.arange(256, dtype=jnp.int32)
    first, second = n // 64, n // 16 % 4
    y_by, z_by = jnp.where(core == 0, first, second), jnp.where(core == 0, second, first)
    token_of_row = 64 * ((y + y_by) % 4) + 16 * ((z + z_by) % 4) + n % 16
    token_of_near = 64 * ((chip + n // 64) % 4) + 32 * (core ^ (n // 32 % 2)) + n % 32
    turn = (token_of_row[:, None] == token_of_near[None, :]).astype(BF16)
    wgu, wd, bo, dif = gate_up_weight, down_weight, gate_up_output_factor, down_input_factor.T
    dof = down_output_factor
    a_both = jnp.concatenate([gate_up_input_factor[0], gate_up_input_factor[1]], 1)
    rows, *part_a = first_half(turn, near, wgu, wd, a_both, dof)
    part_b = second_half(rows, wgu, wd)
    half_a = summed(exchanged(part_a, 0))
    half_b = summed(exchanged(part_b, 0))
    mid_a = middles(exchanged(half_a, 1), bo, dif)
    mid_b = middles(exchanged(half_b, 1), bo, dif, mid_a)
    all_a = collected(stacked(collected(mid_a, 1)), 0)
    all_b = collected(stacked(collected(mid_b, 1)), 0)

    t = T
    halves = third_half(all_a, wgu, wd, bo, dif)
    sums, sent = fourth_half(all_b, wgu, wd, bo, dif, dof, turn, *halves)
    arrived = other_core(sent)
    *everything, arrived = lax.optimization_barrier((*all_a, *all_b, arrived))
    sums = (sums.astype(F32) + arrived.astype(F32)).astype(BF16)
    small, large = sums[..., :256], sums[..., 256:]
    small_sum, large_sum = small.astype(F32), large[0].astype(F32)
    for k in (1, 3, 2):
        sent = jnp.concatenate([large[k]] + [small[j] for j in range(4)], 1)
        got = to_chip(sent, k)
        large_sum = large_sum + got[:, :1024].astype(F32)
        theirs = [got[:, 1024 + 256 * j : 1280 + 256 * j] for j in range(4)]
        small_sum = small_sum + jnp.stack([theirs[(j + k) % 4] for j in range(4)]).astype(F32)
    small_sum = small_sum.astype(BF16)
    small_all = jnp.stack([small_sum, other_core(small_sum)], 1).reshape(256, 256)
    back_low_all, low_down_all = small_all[:, :128], small_all[:, 128:192]

    output = large_sum[:, :512].astype(BF16)
    back_low = small_sum[0][:, :128]
    input_grad = (large_sum[:, 512:] + adapter_scale * dot(back_low, a_both, t)).astype(BF16)
    lower = scale * dot(near[:, :512], back_low_all, ((0,), (0,)))
    grad_gate_up_lower = jnp.stack([lower[:, :64], lower[:, 64:]])
    down_output_factor_gradient = scale * dot(low_down_all, near[:, 512:], ((0,), (0,)))
    gate_up_output_factor_gradient, down_input_factor_gradient = factor_gradients(
        everything[:4], everything[4:]
    )
    return (
        output,
        input_grad,
        grad_gate_up_lower,
        gate_up_output_factor_gradient,
        down_input_factor_gradient,
        down_output_factor_gradient,
    )


def solution(mesh):
    torus = Mesh(mesh.devices.reshape(mesh.shape["dp"], 4, 4), ("dp", "y", "z"))
    mp = ("y", "z")
    in_specs = (
        P("dp", mp),
        P(None, mp, "dp"),
        P("dp", mp),
        P(None, mp, None),
        P(None, None, "dp"),
        P("dp", None),
        P(None, mp),
        P("dp", mp),
    )
    out_specs = (
        P("dp", mp),
        P("dp", mp),
        P(None, mp, None),
        P(None, None, "dp"),
        P("dp", None),
        P(None, mp),
    )
    return jax.shard_map(
        per_device, mesh=torus, in_specs=in_specs, out_specs=out_specs, check_vma=False
    )
```

```python
import jax
import jax.numpy as jnp
from jax import lax
from jax.experimental import pallas as pl
from jax.experimental.pallas import tpu as pltpu
from jax.sharding import Mesh
from jax.sharding import PartitionSpec as P

F32 = jnp.float32
BF16 = jnp.bfloat16
adapter_scale = 2.0
CUT = 896


def other_core(x):
    return lax.ppermute(x, "dp", [(i, i ^ 1) for i in range(lax.axis_size("dp"))])


def to_chip(x, by):
    n = lax.axis_size("dp")
    return lax.ppermute(x, "dp", [(i, (i + 2 * by) % n) for i in range(n)])


def dot(a, b, dims=((1,), (0,))):
    return lax.dot_general(a, b, (dims, ((), ())), preferred_element_type=F32)


def along(x, stage, by):
    pairs = []
    for dp in range(8):
        for y in range(4):
            for z in range(4):
                if (dp + stage) % 2 == 0:
                    there = (y + by) % 4 * 4 + z
                else:
                    there = y * 4 + (z + by) % 4
                pairs.append((dp * 16 + y * 4 + z, dp * 16 + there))
    return lax.ppermute(x, ("dp", "y", "z"), pairs)


def exchanged(blocks, stage):
    return [
        blocks[0],
        along(blocks[1], stage, 1),
        along(blocks[3], stage, -1),
        along(blocks[2], stage, 2),
    ]


def collected(block, stage):
    return [block, along(block, stage, -1), along(block, stage, 2), along(block, stage, 1)]


def whole(n):
    return [pl.BlockSpec(memory_space=pltpu.VMEM)] * n


def in_vmem(shape, dtype):
    return pltpu.VMEM(shape, dtype)


T = ((1,), (1,))


def tiles(lo, hi, step=384):
    return [(a, min(a + step, hi)) for a in range(lo, hi, step)]


def store_blocks(outs, at, value):
    for k in range(4):
        rows = value[64 * k : 64 * k + 64].astype(outs[k].dtype)
        outs[k][:, at : at + value.shape[1]] = rows


def pack_kernel(tokens, cotangent, out, sems):
    copies = [
        pltpu.make_async_copy(tokens, out.at[:, :512], sems.at[0]),
        pltpu.make_async_copy(cotangent, out.at[:, 512:], sems.at[1]),
    ]
    for copy in copies:
        copy.start()
    for copy in copies:
        copy.wait()


def packed(tokens, cotangent):
    return pl.pallas_call(
        pack_kernel,
        out_shape=in_vmem((32, 1024), BF16),
        in_specs=[pl.BlockSpec(memory_space=pltpu.HBM)] * 2,
        out_specs=whole(1)[0],
        scratch_shapes=[pltpu.SemaphoreType.DMA((2,))],
        compiler_params=pltpu.CompilerParams(vmem_limit_bytes=2**20),
        cost_estimate=pl.CostEstimate(flops=10**6, bytes_accessed=10**5, transcendentals=0),
    )(tokens, cotangent)


def load_kernel(*refs):
    n = len(refs) // 2
    copies = [pltpu.make_async_copy(refs[k], refs[n + k], refs[-1].at[k]) for k in range(n)]
    for copy in copies:
        copy.start()
    for copy in copies:
        copy.wait()


def loaded(*arrays):
    return pl.pallas_call(
        load_kernel,
        out_shape=[in_vmem(a.shape, a.dtype) for a in arrays],
        in_specs=[pl.BlockSpec(memory_space=pltpu.HBM)] * len(arrays),
        out_specs=whole(len(arrays)),
        scratch_shapes=[pltpu.SemaphoreType.DMA((len(arrays),))],
        compiler_params=pltpu.CompilerParams(vmem_limit_bytes=2**20),
        cost_estimate=cost(2 * 10**9),
    )(*arrays)


def first_kernel(turn, near, wgu, wd, a_both, dof, rows, *outs):
    rows[...] = dot(turn[...], near[...]).astype(BF16)
    x, c = rows[:, :512], rows[:, 512:]
    store_blocks(outs, 0, dot(x, a_both[...], T))
    store_blocks(outs, 128, dot(c, dof[...], T))
    store_blocks(outs, 192, jnp.zeros((256, 64), F32))
    for k in range(2):
        for lo, hi in tiles(0, CUT):
            store_blocks(outs, 256 + k * CUT + lo, dot(x, wgu[k, :, lo:hi]))
    for lo, hi in tiles(0, CUT):
        store_blocks(outs, 256 + 2 * CUT + lo, dot(c, wd[lo:hi, :], T))


def first_half(turn, near, wgu, wd, a_both, dof):
    shape = (64, 256 + 3 * CUT)
    return pl.pallas_call(
        first_kernel,
        out_shape=[in_vmem((256, 1024), BF16), in_vmem(shape, F32)] + [in_vmem(shape, BF16)] * 3,
        in_specs=whole(6),
        out_specs=whole(5),
        compiler_params=pltpu.CompilerParams(vmem_limit_bytes=12 * 2**20),
        cost_estimate=pl.CostEstimate(flops=10**9, bytes_accessed=10**6, transcendentals=0),
    )(turn, near, wgu, wd, a_both, dof)


def second_kernel(rows, wgu, wd, *outs):
    x, c = rows[:, :512], rows[:, 512:]
    n = 1920 - CUT
    for k in range(2):
        for lo, hi in tiles(CUT, 1920):
            store_blocks(outs, k * n + lo - CUT, dot(x, wgu[k, :, lo:hi]))
    for lo, hi in tiles(CUT, 1920):
        store_blocks(outs, 2 * n + lo - CUT, dot(c, wd[lo:hi, :], T))


def second_half(rows, wgu, wd):
    shape = (64, 3 * (1920 - CUT))
    return pl.pallas_call(
        second_kernel,
        out_shape=[in_vmem(shape, F32)] + [in_vmem(shape, BF16)] * 3,
        in_specs=whole(3),
        out_specs=whole(4),
        compiler_params=pltpu.CompilerParams(vmem_limit_bytes=12 * 2**20),
        cost_estimate=pl.CostEstimate(flops=10**9, bytes_accessed=10**6, transcendentals=0),
    )(rows, wgu, wd)


def params(mib=12):
    return pltpu.CompilerParams(vmem_limit_bytes=mib * 2**20)


def cost(flops):
    return pl.CostEstimate(flops=flops, bytes_accessed=10**6, transcendentals=0)


def total(refs):
    return (
        refs[0][...].astype(F32)
        + refs[1][...].astype(F32)
        + refs[2][...].astype(F32)
        + refs[3][...].astype(F32)
    )


def sum_kernel(*refs):
    value = total(refs[:4])
    for k in range(4):
        out = refs[4 + k]
        out[...] = value[16 * k : 16 * k + 16].astype(out.dtype)


def summed(blocks):
    shape = (16, blocks[0].shape[1])
    return pl.pallas_call(
        sum_kernel,
        out_shape=[in_vmem(shape, F32)] + [in_vmem(shape, BF16)] * 3,
        in_specs=whole(4),
        out_specs=whole(4),
        compiler_params=params(),
        cost_estimate=cost(10**7),
    )(*blocks)


def middle(low, back_down, value, at, lo, hi, bo, dif, out):
    w = hi - lo
    low = low.astype(BF16)
    gate = value[:, at : at + w] + adapter_scale * dot(low[:, :64], bo[0, :, lo:hi])
    up = value[:, at + w : at + 2 * w] + adapter_scale * dot(low[:, 64:], bo[1, :, lo:hi])
    back = value[:, at + 2 * w :] + adapter_scale * dot(back_down, dif[:, lo:hi])
    s = jax.nn.sigmoid(gate)
    out[:, at : at + w] = (gate * s * up).astype(BF16)
    out[:, at + w : at + 2 * w] = (back * up * s * (1.0 + gate * (1.0 - s))).astype(BF16)
    out[:, at + 2 * w :] = (back * gate * s).astype(BF16)


def middle_first_kernel(a, b, c, d, bo, dif, out):
    value = total((a, b, c, d))
    small = value[:, :256].astype(BF16)
    out[:, :256] = small
    middle(value[:, :128], small[:, 128:192], value, 256, 0, CUT, bo, dif, out)


def middle_second_kernel(a, b, c, d, first, bo, dif, out):
    value = total((a, b, c, d))
    middle(first[:, :128], first[:, 128:192], value, 0, CUT, 1920, bo, dif, out)


def middles(blocks, bo, dif, first=None):
    more = [] if first is None else [first]
    return pl.pallas_call(
        middle_first_kernel if first is None else middle_second_kernel,
        out_shape=in_vmem(blocks[0].shape, BF16),
        in_specs=whole(6 + len(more)),
        out_specs=whole(1)[0],
        compiler_params=params(),
        cost_estimate=cost(10**8),
    )(*blocks, *more, bo, dif)


def stack_kernel(a, b, c, d, out):
    for k, ref in enumerate((a, b, c, d)):
        out[16 * k : 16 * k + 16] = ref[...]


def stacked(blocks):
    return pl.pallas_call(
        stack_kernel,
        out_shape=in_vmem((64, blocks[0].shape[1]), BF16),
        in_specs=whole(4),
        out_specs=whole(1)[0],
        compiler_params=params(),
        cost_estimate=cost(10**7),
    )(*blocks)


def joined(refs, lo, hi):
    return jnp.concatenate([ref[:, lo:hi] for ref in refs], 0)


def factor_kernel(*refs):
    a, b, bo_grad, dif_grad = refs[:4], refs[4:8], refs[8], refs[9]
    n = ((0,), (0,))
    scale = adapter_scale * 256 ** (-0.5)
    small = joined(a, 0, 256)
    low, back_down = small[:, :128], small[:, 128:192]
    for part, at, lo, hi in ((a, 256, 0, CUT), (b, 0, CUT, 1920)):
        w = hi - lo
        dif_grad[:, lo:hi] = scale * dot(back_down, joined(part, at, at + w), n)
        for k in range(2):
            g = joined(part, at + (k + 1) * w, at + (k + 2) * w)
            bo_grad[k, :, lo:hi] = scale * dot(low[:, 64 * k : 64 * k + 64], g, n)


def factor_gradients(a, b):
    return pl.pallas_call(
        factor_kernel,
        out_shape=[
            jax.ShapeDtypeStruct((2, 64, 1920), F32),
            jax.ShapeDtypeStruct((64, 1920), F32),
        ],
        in_specs=whole(8),
        out_specs=whole(2),
        compiler_params=params(16),
        cost_estimate=cost(4 * 10**9),
    )(*a, *b)


def back_products(g, at, lo, hi, wgu, wd, bo, dif):
    w = hi - lo
    hidden, gate, up = (joined(g, at + k * w, at + (k + 1) * w) for k in range(3))
    return (
        dot(gate, bo[0, :, lo:hi], T),
        dot(up, bo[1, :, lo:hi], T),
        dot(hidden, dif[:, lo:hi], T),
        dot(hidden, wd[lo:hi, :]),
        dot(gate, wgu[0, :, lo:hi], T) + dot(up, wgu[1, :, lo:hi], T),
    )


def third_kernel(a, b, c, d, wgu, wd, bo, dif, small, out, grad):
    bl0, bl1, ld, o, g = back_products((a, b, c, d), 256, 0, CUT, wgu, wd, bo, dif)
    small[:, :64] = bl0
    small[:, 64:128] = bl1
    small[:, 128:192] = ld
    out[...] = o
    grad[...] = g


def third_half(g, wgu, wd, bo, dif):
    return pl.pallas_call(
        third_kernel,
        out_shape=[
            in_vmem((256, 256), F32),
            in_vmem((256, 512), F32),
            in_vmem((256, 512), F32),
        ],
        in_specs=whole(8),
        out_specs=whole(3),
        compiler_params=params(),
        cost_estimate=cost(10**9),
    )(*g, wgu, wd, bo, dif)


def fourth_kernel(a, b, c, d, wgu, wd, bo, dif, dof, turn, small, out, grad, mine, theirs):
    bl0, bl1, ld, o, g = back_products((a, b, c, d), 0, CUT, 1920, wgu, wd, bo, dif)
    low_down = small[:, 128:192] + ld
    o = o + out[...] + adapter_scale * dot(low_down.astype(BF16), dof[...])

    def put(value, at):
        value = dot(turn[...], value.astype(BF16), ((0,), (0,)))
        for k in range(4):
            mine[k, :, at : at + value.shape[1]] = value[64 * k : 64 * k + 32]
            theirs[k, :, at : at + value.shape[1]] = value[64 * k + 32 : 64 * k + 64].astype(BF16)

    put(small[:, :64] + bl0, 0)
    put(small[:, 64:128] + bl1, 64)
    put(low_down, 128)
    put(jnp.zeros((256, 64), F32), 192)
    put(o, 256)
    put(g + grad[...], 768)


def fourth_half(g, wgu, wd, bo, dif, dof, turn, small, out, grad):
    shape = (4, 32, 1280)
    return pl.pallas_call(
        fourth_kernel,
        out_shape=[in_vmem(shape, F32), in_vmem(shape, BF16)],
        in_specs=whole(13),
        out_specs=whole(2),
        compiler_params=params(),
        cost_estimate=cost(10**9),
    )(*g, wgu, wd, bo, dif, dof, turn, small, out, grad)


def core_sum_kernel(mine, theirs, own, one, two, three):
    value = [mine[k] + theirs[k].astype(F32) for k in range(4)]
    own[:, :1024] = value[0][:, 256:]
    for j in range(4):
        own[:, 1024 + 256 * j : 1280 + 256 * j] = value[j][:, :256]
    value = [v.astype(BF16) for v in value]
    for k, out in ((1, one), (2, two), (3, three)):
        out[:, :1024] = value[k][:, 256:]
        for j in range(4):
            out[:, 1024 + 256 * j : 1280 + 256 * j] = value[(j + k) % 4][:, :256]


def core_sums(mine, theirs):
    shape = (32, 2048)
    return pl.pallas_call(
        core_sum_kernel,
        out_shape=[in_vmem(shape, F32)] + [in_vmem(shape, BF16)] * 3,
        in_specs=whole(2),
        out_specs=whole(4),
        compiler_params=params(),
        cost_estimate=cost(10**7),
    )(mine, theirs)


def chip_sum_kernel(own, a, b, c, small, large):
    value = (
        own[...].astype(F32) + a[...].astype(F32) + b[...].astype(F32) + c[...].astype(F32)
    )
    large[...] = value[:, :1024]
    for j in range(4):
        small[j] = value[:, 1024 + 256 * j : 1280 + 256 * j].astype(BF16)


def chip_sums(own, got):
    return pl.pallas_call(
        chip_sum_kernel,
        out_shape=[in_vmem((4, 32, 256), BF16), in_vmem((32, 1024), F32)],
        in_specs=whole(4),
        out_specs=whole(2),
        compiler_params=params(),
        cost_estimate=cost(10**7),
    )(own, *got)


def finish_kernel(mine, theirs, large, near, a_both, output, input_grad, lower, dof_grad):
    n = ((0,), (0,))
    scale = adapter_scale * 256 ** (-0.5)
    small = jnp.concatenate([r for k in range(4) for r in (mine[k], theirs[k])], 0)
    lower[...] = scale * dot(small[:, :128], near[:, :512], n)
    dof_grad[...] = scale * dot(small[:, 128:192], near[:, 512:], n)
    output[...] = large[:, :512].astype(BF16)
    low = dot(mine[0, :, :128], a_both[...])
    input_grad[...] = (large[:, 512:] + adapter_scale * low).astype(BF16)


def finished(mine, theirs, large, near, a_both):
    return pl.pallas_call(
        finish_kernel,
        out_shape=[
            jax.ShapeDtypeStruct((32, 512), BF16),
            jax.ShapeDtypeStruct((32, 512), BF16),
            jax.ShapeDtypeStruct((128, 512), F32),
            jax.ShapeDtypeStruct((64, 512), F32),
        ],
        in_specs=whole(5),
        out_specs=whole(4),
        compiler_params=params(),
        cost_estimate=cost(10**8),
    )(mine, theirs, large, near, a_both)


def on_device(
    tokens,
    gate_up_weight,
    down_weight,
    gate_up_input_factor,
    gate_up_output_factor,
    down_input_factor,
    down_output_factor,
    cotangent,
):
    dp = lax.axis_index("dp")
    chip, core = dp // 2, dp % 2
    y, z = lax.axis_index("y"), lax.axis_index("z")

    mine = packed(tokens, cotangent)
    a_raw = gate_up_input_factor.transpose(0, 2, 1).reshape(128, 512)
    pair = jnp.concatenate([mine, other_core(mine)], 0)
    near = [pair, to_chip(pair, -1), to_chip(pair, 2), to_chip(pair, 1)]
    near = jnp.concatenate(near, 0)
    wgu1, wd1, a_both, dof = loaded(
        gate_up_weight, down_weight, a_raw, down_output_factor
    )

    n = jnp.arange(256, dtype=jnp.int32)
    first, second = n // 64, n // 16 % 4
    y_by, z_by = jnp.where(core == 0, first, second), jnp.where(core == 0, second, first)
    token_of_row = 64 * ((y + y_by) % 4) + 16 * ((z + z_by) % 4) + n % 16
    token_of_near = 64 * ((chip + n // 64) % 4) + 32 * (core ^ (n // 32 % 2)) + n % 32
    turn = (token_of_row[:, None] == token_of_near[None, :]).astype(BF16)
    wgu, wd, bo, dif = gate_up_weight, down_weight, gate_up_output_factor, down_input_factor.T
    rows, *part_a = first_half(turn, near, wgu1, wd1, a_both, dof)
    part_b = second_half(rows, wgu1, wd1)
    half_a = summed(exchanged(part_a, 0))
    half_b = summed(exchanged(part_b, 0))
    mid_a = middles(exchanged(half_a, 1), bo, dif)
    mid_b = middles(exchanged(half_b, 1), bo, dif, mid_a)
    all_a = collected(stacked(collected(mid_a, 1)), 0)
    all_b = collected(stacked(collected(mid_b, 1)), 0)

    halves = third_half(all_a, wgu, wd, bo, dif)
    sums, sent = fourth_half(all_b, wgu, wd, bo, dif, down_output_factor, turn, *halves)
    arrived = other_core(sent)
    *everything, arrived = lax.optimization_barrier((*all_a, *all_b, arrived))
    gate_up_output_factor_gradient, down_input_factor_gradient = factor_gradients(
        everything[:4], everything[4:]
    )
    own, *sent = core_sums(sums, arrived)
    got = [to_chip(sent[0], 1), to_chip(sent[2], 3), to_chip(sent[1], 2)]
    small, large = chip_sums(own, got)
    output, input_grad, lower, down_output_factor_gradient = finished(
        small, other_core(small), large, near, a_raw
    )
    grad_gate_up_lower = lower.reshape(2, 64, 512).transpose(0, 2, 1)
    return (
        output,
        input_grad,
        grad_gate_up_lower,
        gate_up_output_factor_gradient,
        down_input_factor_gradient.T,
        down_output_factor_gradient,
    )


def solution(mesh):
    torus = Mesh(mesh.devices.reshape(mesh.shape["dp"], 4, 4), ("dp", "y", "z"))
    mp = ("y", "z")
    in_specs = (
        P("dp", mp),
        P(None, mp, "dp"),
        P("dp", mp),
        P(None, mp, None),
        P(None, None, "dp"),
        P("dp", None),
        P(None, mp),
        P("dp", mp),
    )
    out_specs = (
        P("dp", mp),
        P("dp", mp),
        P(None, mp, None),
        P(None, None, "dp"),
        P("dp", None),
        P(None, mp),
    )
    return jax.shard_map(
        on_device, mesh=torus, in_specs=in_specs, out_specs=out_specs, check_vma=False
    )
```

```python
import jax
import jax.numpy as jnp
from jax import lax
from jax.experimental import pallas as pl
from jax.experimental.pallas import tpu as pltpu
from jax.sharding import Mesh
from jax.sharding import PartitionSpec as P

F32 = jnp.float32
BF16 = jnp.bfloat16
adapter_scale = 2.0
CUT = 896


def other_core(x):
    return lax.ppermute(x, "dp", [(i, i ^ 1) for i in range(lax.axis_size("dp"))])


def to_chip(x, by):
    n = lax.axis_size("dp")
    return lax.ppermute(x, "dp", [(i, (i + 2 * by) % n) for i in range(n)])


def dot(a, b, dims=((1,), (0,))):
    return lax.dot_general(a, b, (dims, ((), ())), preferred_element_type=F32)


def along(x, stage, by):
    pairs = []
    for dp in range(8):
        for y in range(4):
            for z in range(4):
                if (dp + stage) % 2 == 0:
                    there = (y + by) % 4 * 4 + z
                else:
                    there = y * 4 + (z + by) % 4
                pairs.append((dp * 16 + y * 4 + z, dp * 16 + there))
    return lax.ppermute(x, ("dp", "y", "z"), pairs)


def exchanged(blocks, stage):
    return [
        blocks[0],
        along(blocks[1], stage, 1),
        along(blocks[3], stage, -1),
        along(blocks[2], stage, 2),
    ]


def collected(block, stage):
    return [block, along(block, stage, -1), along(block, stage, 2), along(block, stage, 1)]


def whole(n):
    return [pl.BlockSpec(memory_space=pltpu.VMEM)] * n


def in_vmem(shape, dtype):
    return pltpu.VMEM(shape, dtype)


T = ((1,), (1,))


def tiles(lo, hi, step=384):
    return [(a, min(a + step, hi)) for a in range(lo, hi, step)]


def store_blocks(outs, at, value):
    for k in range(4):
        rows = value[64 * k : 64 * k + 64].astype(outs[k].dtype)
        outs[k][:, at : at + value.shape[1]] = rows


def pack_kernel(tokens, cotangent, out, sems):
    copies = [
        pltpu.make_async_copy(tokens, out.at[:, :512], sems.at[0]),
        pltpu.make_async_copy(cotangent, out.at[:, 512:], sems.at[1]),
    ]
    for copy in copies:
        copy.start()
    for copy in copies:
        copy.wait()


def packed(tokens, cotangent):
    return pl.pallas_call(
        pack_kernel,
        out_shape=in_vmem((32, 1024), BF16),
        in_specs=[pl.BlockSpec(memory_space=pltpu.HBM)] * 2,
        out_specs=whole(1)[0],
        scratch_shapes=[pltpu.SemaphoreType.DMA((2,))],
        compiler_params=pltpu.CompilerParams(vmem_limit_bytes=2**20),
        cost_estimate=pl.CostEstimate(flops=10**6, bytes_accessed=10**5, transcendentals=0),
    )(tokens, cotangent)


def load_kernel(*refs):
    n = len(refs) // 2
    copies = [pltpu.make_async_copy(refs[k], refs[n + k], refs[-1].at[k]) for k in range(n)]
    for copy in copies:
        copy.start()
    for copy in copies:
        copy.wait()


def loaded(*arrays):
    return pl.pallas_call(
        load_kernel,
        out_shape=[in_vmem(a.shape, a.dtype) for a in arrays],
        in_specs=[pl.BlockSpec(memory_space=pltpu.HBM)] * len(arrays),
        out_specs=whole(len(arrays)),
        scratch_shapes=[pltpu.SemaphoreType.DMA((len(arrays),))],
        compiler_params=pltpu.CompilerParams(vmem_limit_bytes=2**20),
        cost_estimate=cost(2 * 10**9),
    )(*arrays)


def first_kernel(turn, near, wgu, wd, a_both, dof, rows, *outs):
    rows[...] = dot(turn[...], near[...]).astype(BF16)
    x, c = rows[:, :512], rows[:, 512:]
    store_blocks(outs, 0, dot(x, a_both[...], T))
    store_blocks(outs, 128, dot(c, dof[...], T))
    store_blocks(outs, 192, jnp.zeros((256, 64), F32))
    for k in range(2):
        for lo, hi in tiles(0, CUT):
            store_blocks(outs, 256 + k * CUT + lo, dot(x, wgu[k, :, lo:hi]))
    for lo, hi in tiles(0, CUT):
        store_blocks(outs, 256 + 2 * CUT + lo, dot(c, wd[lo:hi, :], T))


def first_half(turn, near, wgu, wd, a_both, dof):
    shape = (64, 256 + 3 * CUT)
    return pl.pallas_call(
        first_kernel,
        out_shape=[in_vmem((256, 1024), BF16), in_vmem(shape, F32)] + [in_vmem(shape, BF16)] * 3,
        in_specs=whole(6),
        out_specs=whole(5),
        compiler_params=pltpu.CompilerParams(vmem_limit_bytes=12 * 2**20),
        cost_estimate=pl.CostEstimate(flops=10**9, bytes_accessed=10**6, transcendentals=0),
    )(turn, near, wgu, wd, a_both, dof)


def second_kernel(rows, wgu, wd, *outs):
    x, c = rows[:, :512], rows[:, 512:]
    n = 1920 - CUT
    for k in range(2):
        for lo, hi in tiles(CUT, 1920):
            store_blocks(outs, k * n + lo - CUT, dot(x, wgu[k, :, lo:hi]))
    for lo, hi in tiles(CUT, 1920):
        store_blocks(outs, 2 * n + lo - CUT, dot(c, wd[lo:hi, :], T))


def second_half(rows, wgu, wd):
    shape = (64, 3 * (1920 - CUT))
    return pl.pallas_call(
        second_kernel,
        out_shape=[in_vmem(shape, F32)] + [in_vmem(shape, BF16)] * 3,
        in_specs=whole(3),
        out_specs=whole(4),
        compiler_params=pltpu.CompilerParams(vmem_limit_bytes=12 * 2**20),
        cost_estimate=pl.CostEstimate(flops=10**9, bytes_accessed=10**6, transcendentals=0),
    )(rows, wgu, wd)


def params(mib=12):
    return pltpu.CompilerParams(vmem_limit_bytes=mib * 2**20)


def cost(flops):
    return pl.CostEstimate(flops=flops, bytes_accessed=10**6, transcendentals=0)


def total(refs):
    return (
        refs[0][...].astype(F32)
        + refs[1][...].astype(F32)
        + refs[2][...].astype(F32)
        + refs[3][...].astype(F32)
    )


def sum_kernel(*refs):
    value = total(refs[:4])
    for k in range(4):
        out = refs[4 + k]
        out[...] = value[16 * k : 16 * k + 16].astype(out.dtype)


def summed(blocks):
    shape = (16, blocks[0].shape[1])
    return pl.pallas_call(
        sum_kernel,
        out_shape=[in_vmem(shape, F32)] + [in_vmem(shape, BF16)] * 3,
        in_specs=whole(4),
        out_specs=whole(4),
        compiler_params=params(),
        cost_estimate=cost(10**7),
    )(*blocks)


def middle(low, back_down, value, at, lo, hi, bo, dif, out):
    w = hi - lo
    low = low.astype(BF16)
    gate = value[:, at : at + w] + adapter_scale * dot(low[:, :64], bo[0, :, lo:hi])
    up = value[:, at + w : at + 2 * w] + adapter_scale * dot(low[:, 64:], bo[1, :, lo:hi])
    back = value[:, at + 2 * w :] + adapter_scale * dot(back_down, dif[:, lo:hi])
    s = jax.nn.sigmoid(gate)
    out[:, at : at + w] = (gate * s * up).astype(BF16)
    out[:, at + w : at + 2 * w] = (back * up * s * (1.0 + gate * (1.0 - s))).astype(BF16)
    out[:, at + 2 * w :] = (back * gate * s).astype(BF16)


def middle_first_kernel(a, b, c, d, bo, dif, out):
    value = total((a, b, c, d))
    small = value[:, :256].astype(BF16)
    out[:, :256] = small
    middle(value[:, :128], small[:, 128:192], value, 256, 0, CUT, bo, dif, out)


def middle_second_kernel(a, b, c, d, first, bo, dif, out):
    value = total((a, b, c, d))
    middle(first[:, :128], first[:, 128:192], value, 0, CUT, 1920, bo, dif, out)


def middles(blocks, bo, dif, first=None):
    more = [] if first is None else [first]
    return pl.pallas_call(
        middle_first_kernel if first is None else middle_second_kernel,
        out_shape=in_vmem(blocks[0].shape, BF16),
        in_specs=whole(6 + len(more)),
        out_specs=whole(1)[0],
        compiler_params=params(),
        cost_estimate=cost(10**8),
    )(*blocks, *more, bo, dif)


def stack_kernel(a, b, c, d, out):
    for k, ref in enumerate((a, b, c, d)):
        out[16 * k : 16 * k + 16] = ref[...]


def stacked(blocks):
    return pl.pallas_call(
        stack_kernel,
        out_shape=in_vmem((64, blocks[0].shape[1]), BF16),
        in_specs=whole(4),
        out_specs=whole(1)[0],
        compiler_params=params(),
        cost_estimate=cost(10**7),
    )(*blocks)


def joined(refs, lo, hi):
    return jnp.concatenate([ref[:, lo:hi] for ref in refs], 0)


def factor_kernel(*refs):
    a, b, bo_grad, dif_grad = refs[:4], refs[4:8], refs[8], refs[9]
    n = ((0,), (0,))
    scale = adapter_scale * 256 ** (-0.5)
    small = joined(a, 0, 256)
    low, back_down = small[:, :128], small[:, 128:192]
    for part, at, lo, hi in ((a, 256, 0, CUT), (b, 0, CUT, 1920)):
        w = hi - lo
        dif_grad[:, lo:hi] = scale * dot(back_down, joined(part, at, at + w), n)
        for k in range(2):
            g = joined(part, at + (k + 1) * w, at + (k + 2) * w)
            bo_grad[k, :, lo:hi] = scale * dot(low[:, 64 * k : 64 * k + 64], g, n)


def factor_gradients(a, b):
    return pl.pallas_call(
        factor_kernel,
        out_shape=[
            jax.ShapeDtypeStruct((2, 64, 1920), F32),
            jax.ShapeDtypeStruct((64, 1920), F32),
        ],
        in_specs=whole(8),
        out_specs=whole(2),
        compiler_params=params(16),
        cost_estimate=cost(4 * 10**9),
    )(*a, *b)


def back_products(g, at, lo, hi, wgu, wd, bo, dif):
    w = hi - lo
    hidden, gate, up = (joined(g, at + k * w, at + (k + 1) * w) for k in range(3))
    return (
        dot(gate, bo[0, :, lo:hi], T),
        dot(up, bo[1, :, lo:hi], T),
        dot(hidden, dif[:, lo:hi], T),
        dot(hidden, wd[lo:hi, :]),
        dot(gate, wgu[0, :, lo:hi], T) + dot(up, wgu[1, :, lo:hi], T),
    )


def third_kernel(a, b, c, d, wgu, wd, bo, dif, small, out, grad):
    bl0, bl1, ld, o, g = back_products((a, b, c, d), 256, 0, CUT, wgu, wd, bo, dif)
    small[:, :64] = bl0
    small[:, 64:128] = bl1
    small[:, 128:192] = ld
    out[...] = o
    grad[...] = g


def third_half(g, wgu, wd, bo, dif):
    return pl.pallas_call(
        third_kernel,
        out_shape=[
            in_vmem((256, 256), F32),
            in_vmem((256, 512), F32),
            in_vmem((256, 512), F32),
        ],
        in_specs=whole(8),
        out_specs=whole(3),
        compiler_params=params(),
        cost_estimate=cost(10**9),
    )(*g, wgu, wd, bo, dif)


def fourth_kernel(a, b, c, d, wgu, wd, bo, dif, dof, turn, small, out, grad, mine, theirs):
    bl0, bl1, ld, o, g = back_products((a, b, c, d), 0, CUT, 1920, wgu, wd, bo, dif)
    low_down = small[:, 128:192] + ld
    o = o + out[...] + adapter_scale * dot(low_down.astype(BF16), dof[...])

    def put(value, at):
        value = dot(turn[...], value.astype(BF16), ((0,), (0,)))
        for k in range(4):
            mine[k, :, at : at + value.shape[1]] = value[64 * k : 64 * k + 32]
            theirs[k, :, at : at + value.shape[1]] = value[64 * k + 32 : 64 * k + 64].astype(BF16)

    put(small[:, :64] + bl0, 0)
    put(small[:, 64:128] + bl1, 64)
    put(low_down, 128)
    put(jnp.zeros((256, 64), F32), 192)
    put(o, 256)
    put(g + grad[...], 768)


def fourth_half(g, wgu, wd, bo, dif, dof, turn, small, out, grad):
    shape = (4, 32, 1280)
    return pl.pallas_call(
        fourth_kernel,
        out_shape=[in_vmem(shape, F32), in_vmem(shape, BF16)],
        in_specs=whole(13),
        out_specs=whole(2),
        compiler_params=params(),
        cost_estimate=cost(10**9),
    )(*g, wgu, wd, bo, dif, dof, turn, small, out, grad)


def core_sum_kernel(mine, theirs, own, one, two, three):
    value = [mine[k] + theirs[k].astype(F32) for k in range(4)]
    own[:, :1024] = value[0][:, 256:]
    for j in range(4):
        own[:, 1024 + 192 * j : 1216 + 192 * j] = value[j][:, :192]
    value = [v.astype(BF16) for v in value]
    for k, out in ((1, one), (2, two), (3, three)):
        out[:, :1024] = value[k][:, 256:]
        for j in range(4):
            out[:, 1024 + 192 * j : 1216 + 192 * j] = value[(j + k) % 4][:, :192]


def core_sums(mine, theirs):
    shape = (32, 1792)
    return pl.pallas_call(
        core_sum_kernel,
        out_shape=[in_vmem(shape, F32)] + [in_vmem(shape, BF16)] * 3,
        in_specs=whole(2),
        out_specs=whole(4),
        compiler_params=params(),
        cost_estimate=cost(10**7),
    )(mine, theirs)


def chip_sum_kernel(own, a, b, c, small, large):
    value = (
        own[...].astype(F32) + a[...].astype(F32) + b[...].astype(F32) + c[...].astype(F32)
    )
    large[...] = value[:, :1024]
    for j in range(4):
        small[j] = value[:, 1024 + 192 * j : 1216 + 192 * j].astype(BF16)


def chip_sums(own, got):
    return pl.pallas_call(
        chip_sum_kernel,
        out_shape=[in_vmem((4, 32, 192), BF16), in_vmem((32, 1024), F32)],
        in_specs=whole(4),
        out_specs=whole(2),
        compiler_params=params(),
        cost_estimate=cost(10**7),
    )(own, *got)


def finish_kernel(mine, theirs, large, near, a_both, output, input_grad, lower, dof_grad):
    n = ((0,), (0,))
    scale = adapter_scale * 256 ** (-0.5)
    small = jnp.concatenate([r for k in range(4) for r in (mine[k], theirs[k])], 0)
    lower[...] = scale * dot(small[:, :128], near[:, :512], n)
    dof_grad[...] = scale * dot(small[:, 128:192], near[:, 512:], n)
    output[...] = large[:, :512].astype(BF16)
    low = dot(mine[0, :, :128], a_both[...])
    input_grad[...] = (large[:, 512:] + adapter_scale * low).astype(BF16)


def finished(mine, theirs, large, near, a_both):
    return pl.pallas_call(
        finish_kernel,
        out_shape=[
            jax.ShapeDtypeStruct((32, 512), BF16),
            jax.ShapeDtypeStruct((32, 512), BF16),
            jax.ShapeDtypeStruct((128, 512), F32),
            jax.ShapeDtypeStruct((64, 512), F32),
        ],
        in_specs=whole(5),
        out_specs=whole(4),
        compiler_params=params(),
        cost_estimate=cost(10**8),
    )(mine, theirs, large, near, a_both)


def on_device(
    tokens,
    gate_up_weight,
    down_weight,
    gate_up_input_factor,
    gate_up_output_factor,
    down_input_factor,
    down_output_factor,
    cotangent,
):
    dp = lax.axis_index("dp")
    chip, core = dp // 2, dp % 2
    y, z = lax.axis_index("y"), lax.axis_index("z")

    mine = packed(tokens, cotangent)
    a_raw = gate_up_input_factor.transpose(0, 2, 1).reshape(128, 512)
    pair = jnp.concatenate([mine, other_core(mine)], 0)
    near = [pair, to_chip(pair, -1), to_chip(pair, 2), to_chip(pair, 1)]
    near = jnp.concatenate(near, 0)
    wgu1, wd1, a_both, dof = loaded(
        gate_up_weight, down_weight, a_raw, down_output_factor
    )

    n = jnp.arange(256, dtype=jnp.int32)
    first, second = n // 64, n // 16 % 4
    y_by, z_by = jnp.where(core == 0, first, second), jnp.where(core == 0, second, first)
    token_of_row = 64 * ((y + y_by) % 4) + 16 * ((z + z_by) % 4) + n % 16
    token_of_near = 64 * ((chip + n // 64) % 4) + 32 * (core ^ (n // 32 % 2)) + n % 32
    turn = (token_of_row[:, None] == token_of_near[None, :]).astype(BF16)
    wgu, wd, bo, dif = gate_up_weight, down_weight, gate_up_output_factor, down_input_factor.T
    rows, *part_a = first_half(turn, near, wgu1, wd1, a_both, dof)
    part_b = second_half(rows, wgu1, wd1)
    half_a = summed(exchanged(part_a, 0))
    half_b = summed(exchanged(part_b, 0))
    mid_a = middles(exchanged(half_a, 1), bo, dif)
    mid_b = middles(exchanged(half_b, 1), bo, dif, mid_a)
    all_a = collected(stacked(collected(mid_a, 1)), 0)
    all_b = collected(stacked(collected(mid_b, 1)), 0)

    halves = third_half(all_a, wgu, wd, bo, dif)
    sums, sent = fourth_half(all_b, wgu, wd, bo, dif, down_output_factor, turn, *halves)
    arrived = other_core(sent)
    *everything, arrived = lax.optimization_barrier((*all_a, *all_b, arrived))
    gate_up_output_factor_gradient, down_input_factor_gradient = factor_gradients(
        everything[:4], everything[4:]
    )
    own, *sent = core_sums(sums, arrived)
    got = [to_chip(sent[0], 1), to_chip(sent[2], 3), to_chip(sent[1], 2)]
    small, large = chip_sums(own, got)
    output, input_grad, lower, down_output_factor_gradient = finished(
        small, other_core(small), large, near, a_raw
    )
    grad_gate_up_lower = lower.reshape(2, 64, 512).transpose(0, 2, 1)
    return (
        output,
        input_grad,
        grad_gate_up_lower,
        gate_up_output_factor_gradient,
        down_input_factor_gradient.T,
        down_output_factor_gradient,
    )


def solution(mesh):
    torus = Mesh(mesh.devices.reshape(mesh.shape["dp"], 4, 4), ("dp", "y", "z"))
    mp = ("y", "z")
    in_specs = (
        P("dp", mp),
        P(None, mp, "dp"),
        P("dp", mp),
        P(None, mp, None),
        P(None, None, "dp"),
        P("dp", None),
        P(None, mp),
        P("dp", mp),
    )
    out_specs = (
        P("dp", mp),
        P("dp", mp),
        P(None, mp, None),
        P(None, None, "dp"),
        P("dp", None),
        P(None, mp),
    )
    return jax.shard_map(
        on_device, mesh=torus, in_specs=in_specs, out_specs=out_specs, check_vma=False
    )
```
